64 devices in a mesh: dp: 4 (over x, y), sp: 16 (over z, core).
Axes of the slice: x: 2, y: 2, z: 8, core: 2. Of those that a mesh axis runs over, the one named last changes fastest.
The devices are a block of a 4x4x8 slice.
Arguments:
- q: bfloat16 [128, 64, 64], P('dp'), parts along dimension 0
- k: bfloat16 [128, 2048, 64, 64], P('dp', 'sp'), parts along dimension 0
- v: bfloat16 [128, 2048, 64, 64], P('dp', 'sp'), parts along dimension 0
Outputs:
- q: bfloat16 [128, 64, 64], P('dp'), parts along dimension 0
There are 4 independent parts. The reference program is written for one: setup_inputs(seed, part) draws one part's arguments, and reference() takes and returns one part's arrays. A program takes and returns all parts, laid end to end along the dimension named above; each array names one.
All inputs are finite; a program needn't handle non-finite values.
Results may differ from the reference program's by a relative error of at most 0.012.
Values are sent between devices in bfloat16 or wider.
A program may use at most 768 MiB of HBM per device.

```python
import jax
import jax.numpy as jnp

BATCH = 32
CACHE = 2048
HEADS = 64
KV_HEADS = 64
HEAD = 64


def setup_inputs(seed: int = 0, part: int = 0) -> dict:
    kq, kk, kv = (jax.random.fold_in(k, part) for k in jax.random.split(jax.random.key(seed), 3))
    return {
        "q": (3 * jax.random.normal(kq, (BATCH, HEADS, HEAD), jnp.float32)).astype(jnp.bfloat16),
        "k": jax.random.normal(kk, (BATCH, CACHE, KV_HEADS, HEAD), jnp.float32).astype(jnp.bfloat16),
        "v": jax.random.normal(kv, (BATCH, CACHE, KV_HEADS, HEAD), jnp.float32).astype(jnp.bfloat16),
    }


def einsum(form, a, b):
    return jnp.einsum(form, a.astype(jnp.float32), b.astype(jnp.float32))


def reference(q, k, v):
    grouped = q.reshape(BATCH, KV_HEADS, -1, HEAD)
    scores = einsum("bgsd,bugd->bgsu", grouped, k) * HEAD**-0.5
    weights = jax.nn.softmax(scores, -1).astype(jnp.bfloat16)
    return einsum("bgsu,bugd->bgsd", weights, v).astype(jnp.bfloat16).reshape(BATCH, HEADS, HEAD)
```

```python
import functools

import jax
import jax.numpy as jnp
from jax import lax
from jax.experimental import pallas as pl
from jax.experimental.pallas import tpu as pltpu
from jax.sharding import PartitionSpec as P

MESH = pl.DeviceIdType.MESH
F32, BF16 = jnp.float32, jnp.bfloat16
SLOTS = 6
ROWS = 16


def iota(shape, dim):
    return lax.broadcasted_iota(jnp.int32, shape, dim)


def scores_of(q, keys, head):
    heads = q.shape[0]
    per = 128 // head
    out = []
    for first in range(0, heads, ROWS):
        rows = q[first : first + ROWS]
        wide = jnp.concatenate([rows] * per, axis=1)
        blocks = [
            jnp.where(iota((ROWS, 128), 0) == iota((ROWS, 128), 1) // head + per * j, wide, jnp.zeros_like(wide))
            for j in range(ROWS // per)
        ]
        out.append(
            jnp.dot(
                jnp.concatenate(blocks, axis=1),
                keys[first * head : (first + ROWS) * head],
                preferred_element_type=F32,
            )
        )
    return jnp.concatenate(out, axis=0) * head**-0.5


def row_of(column, heads):
    own = iota((heads, 128), 1) % heads == iota((heads, 128), 0)
    return jnp.sum(jnp.where(own, column, 0.0), axis=0, keepdims=True)


def weights_of(scores):
    heads, tokens = scores.shape
    high = jnp.max(scores, axis=1, keepdims=True)
    weights = jnp.exp(scores - high)
    total = jnp.sum(weights, axis=1, keepdims=True)
    wide = lambda x: jnp.broadcast_to(x, (heads, 128))
    return weights.astype(BF16), row_of(wide(total), heads), row_of(wide(high), heads)


def seen_of(weights, values, head):
    heads, tokens = weights.shape
    half = heads // 2
    nothing = jnp.zeros((half, tokens), BF16)
    lower = jnp.concatenate([weights[:half], nothing] * (128 // heads), axis=0)
    upper = jnp.concatenate([nothing, weights[half:]] * (128 // heads), axis=0)
    both = jnp.concatenate([values[: half * head], values[half * head :]], axis=1)
    products = lax.dot_general(
        both, jnp.concatenate([lower, upper], axis=1), (((1,), (1,)), ((), ())), preferred_element_type=F32
    )
    lane = iota((head // 2, 128), 1)
    out = jnp.zeros((head // 2, 128), F32)
    for h in range(half):
        mine = products[h * head : (h + 1) * head]
        out = jnp.where(lane % half == h, jnp.where(lane < heads, mine[: head // 2], mine[head // 2 :]), out)
    return out


def kernel(
    n,
    q_ref,
    k_hbm,
    v_hbm,
    out_ref,
    kbuf,
    vbuf,
    part,
    stat,
    parts,
    stats,
    done,
    k_sem,
    v_sem,
    part_send,
    stat_send,
    part_recv,
    stat_recv,
    done_send,
    done_recv,
):
    me = lax.axis_index("sp")
    sequences = k_hbm.shape[0]
    heads = q_ref.shape[0] // sequences
    head = q_ref.shape[1]
    chips = n // 2
    chip, core = me // 2, me % 2

    def owner_of(t):
        j = t // 2
        away = (chips // 2 - (j + 1) // 2) * (2 * (j % 2) - 1)
        return (chip + away + chips) % chips * 2 + (core + 1 + t % 2) % 2

    def sequence_of(i):
        return i // n * n + owner_of(i % n)

    def k_copy(i):
        slot = i % SLOTS
        return pltpu.make_async_copy(k_hbm.at[sequence_of(i)], kbuf.at[slot], k_sem.at[slot])

    def v_copy(i):
        slot = i % SLOTS
        return pltpu.make_async_copy(v_hbm.at[sequence_of(i)], vbuf.at[slot], v_sem.at[slot])

    def part_copies(i):
        to = {"sp": owner_of(i % n)}
        return (
            pltpu.make_async_remote_copy(
                part.at[i], parts.at[i], part_send.at[i], part_recv.at[i], device_id=to, device_id_type=MESH
            ),
            pltpu.make_async_remote_copy(
                stat.at[i], stats.at[i], stat_send.at[i], stat_recv.at[i], device_id=to, device_id_type=MESH
            ),
        )

    def done_copy(r, t):
        mine = r * n + me
        return pltpu.make_async_remote_copy(
            done.at[mine],
            done.at[mine],
            done_send.at[r * n + t],
            done_recv.at[r * n + t],
            device_id={"sp": owner_of(t)},
            device_id_type=MESH,
        )

    def q_of(i):
        return q_ref[pl.ds(pl.multiple_of(sequence_of(i) * heads, heads), heads), :]

    def score(i):
        weights, total, high = weights_of(scores_of(q_of(i), kbuf.at[i % SLOTS], head))
        return weights, total, high

    def keep_stat(i, total, high):
        stat[i] = jnp.concatenate([total, high], axis=0)

    def see(i, weights):
        part[i] = seen_of(weights, vbuf.at[i % SLOTS], head).astype(BF16)

    def finish(r):
        own = r * n + n - 1
        for t in range(n - 1):
            for copy in part_copies(r * n + t):
                copy.wait_recv()
        parts[own] = part[own]
        stats[own] = stat[own]
        highs = [stats[r * n + t][1:2] for t in range(n)]
        high = functools.reduce(jnp.maximum, highs)
        total = jnp.zeros_like(high)
        seen = jnp.zeros(parts.shape[1:], F32)
        for t in range(n):
            scale = jnp.exp(highs[t] - high)
            total += stats[r * n + t][0:1] * scale
            seen += parts[r * n + t].astype(F32) * scale
        done[r * n + me] = (seen / total).astype(BF16)
        for t in range(n - 1):
            done_copy(r, t).start()

    for i in range(SLOTS):
        k_copy(i).start()
        if i < SLOTS - 1:
            v_copy(i).start()
    barrier = pltpu.get_barrier_semaphore()
    for away in range(1, n):
        pl.semaphore_signal(barrier, inc=1, device_id={"sp": (me + away) % n}, device_id_type=MESH)

    k_copy(0).wait()
    weights, total, high = score(0)
    keep_stat(0, total, high)
    pl.semaphore_wait(barrier, n - 1)

    def step(i, weights):
        k_copy(i + 1).wait()
        v_copy(i).wait()

        @pl.when(i + SLOTS < sequences)
        def _():
            k_copy(i + SLOTS).start()

        @pl.when(i + SLOTS - 1 < sequences)
        def _():
            v_copy(i + SLOTS - 1).start()

        @pl.when((i > 0) & (i % n != 0))
        def _():
            for copy in part_copies(i - 1):
                copy.start()

        later, total, high = score(i + 1)
        see(i, weights)
        keep_stat(i + 1, total, high)

        for r in range(sequences // n - 1):

            @pl.when(i == (r + 1) * n + n // 2)
            def _():
                finish(r)

        return later

    weights = lax.fori_loop(0, sequences - 1, step, weights)
    last = sequences - 1
    v_copy(last).wait()
    for copy in part_copies(last - 1):
        copy.start()
    see(last, weights)
    rounds = sequences // n
    finish(rounds - 1)
    for r in range(rounds):
        for t in range(n - 1):
            copy = done_copy(r, t)
            copy.wait_recv()
            copy.wait_send()
            for copy in part_copies(r * n + t):
                copy.wait_send()
    out_ref[...] = done[...]


def solution(mesh):
    n = mesh.shape["sp"]

    def step(q, k, v):
        sequences, tokens, heads, head = k.shape
        keys, values = (jnp.transpose(x, (0, 2, 3, 1)).reshape(sequences, heads * head, tokens) for x in (k, v))
        half = head // 2
        packed = (sequences, half, 2 * heads)
        out = pl.pallas_call(
            functools.partial(kernel, n),
            out_shape=jax.ShapeDtypeStruct(packed, BF16),
            in_specs=[
                pl.BlockSpec(memory_space=pltpu.VMEM),
                pl.BlockSpec(memory_space=pl.ANY),
                pl.BlockSpec(memory_space=pl.ANY),
            ],
            out_specs=pl.BlockSpec(memory_space=pltpu.VMEM),
            scratch_shapes=[
                pltpu.VMEM((SLOTS, heads * head, tokens), BF16),
                pltpu.VMEM((SLOTS, heads * head, tokens), BF16),
                pltpu.VMEM(packed, BF16),
                pltpu.VMEM((sequences, 2, 2 * heads), F32),
                pltpu.VMEM(packed, BF16),
                pltpu.VMEM((sequences, 2, 2 * heads), F32),
                pltpu.VMEM(packed, BF16),
                pltpu.SemaphoreType.DMA((SLOTS,)),
                pltpu.SemaphoreType.DMA((SLOTS,)),
                pltpu.SemaphoreType.DMA((sequences,)),
                pltpu.SemaphoreType.DMA((sequences,)),
                pltpu.SemaphoreType.DMA((sequences,)),
                pltpu.SemaphoreType.DMA((sequences,)),
                pltpu.SemaphoreType.DMA((sequences,)),
                pltpu.SemaphoreType.DMA((sequences,)),
            ],
            compiler_params=pltpu.CompilerParams(collective_id=0, has_side_effects=True),
        )(q.reshape(sequences * heads, head), keys, values)
        return out.reshape(sequences, half, 2, heads).transpose(0, 3, 2, 1).reshape(q.shape)

    return jax.shard_map(
        step,
        mesh=mesh,
        in_specs=(P("dp", None, None), P("dp", "sp", None, None), P("dp", "sp", None, None)),
        out_specs=P("dp", None, None),
        check_vma=False,
    )
```

```python
import functools

import jax
import jax.numpy as jnp
from jax import lax
from jax.experimental import pallas as pl
from jax.experimental.pallas import tpu as pltpu
from jax.sharding import PartitionSpec as P

MESH = pl.DeviceIdType.MESH
F32, BF16 = jnp.float32, jnp.bfloat16
SLOTS = 4
EARLY = 3
ROWS = 16


def iota(shape, dim):
    return lax.broadcasted_iota(jnp.int32, shape, dim)


def scores_of(q, keys, head):
    heads = q.shape[0]
    per = 128 // head
    out = []
    for first in range(0, heads, ROWS):
        rows = q[first : first + ROWS]
        wide = jnp.concatenate([rows] * per, axis=1)
        blocks = [
            jnp.where(iota((ROWS, 128), 0) == iota((ROWS, 128), 1) // head + per * j, wide, jnp.zeros_like(wide))
            for j in range(ROWS // per)
        ]
        out.append(
            jnp.dot(
                jnp.concatenate(blocks, axis=1),
                keys[first * head : (first + ROWS) * head],
                preferred_element_type=F32,
            )
        )
    return jnp.concatenate(out, axis=0) * head**-0.5


def row_of(column, heads):
    own = iota((heads, 128), 1) % heads == iota((heads, 128), 0)
    return jnp.sum(jnp.where(own, column, 0.0), axis=0, keepdims=True)


def weights_of(scores):
    heads, tokens = scores.shape
    high = jnp.max(scores, axis=1, keepdims=True)
    weights = jnp.exp(scores - high)
    total = jnp.sum(weights, axis=1, keepdims=True)
    wide = lambda x: jnp.broadcast_to(x, (heads, 128))
    return weights.astype(BF16), row_of(wide(total), heads), row_of(wide(high), heads)


def seen_of(weights, values, head):
    heads, tokens = weights.shape
    half = heads // 2
    nothing = jnp.zeros((half, tokens), BF16)
    lower = jnp.concatenate([weights[:half], nothing] * (128 // heads), axis=0)
    upper = jnp.concatenate([nothing, weights[half:]] * (128 // heads), axis=0)
    both = jnp.concatenate([values[: half * head], values[half * head :]], axis=1)
    products = lax.dot_general(
        both, jnp.concatenate([lower, upper], axis=1), (((1,), (1,)), ((), ())), preferred_element_type=F32
    )
    lane = iota((head // 2, 128), 1)
    out = jnp.zeros((head // 2, 128), F32)
    for h in range(half):
        mine = products[h * head : (h + 1) * head]
        out = jnp.where(lane % half == h, jnp.where(lane < heads, mine[: head // 2], mine[head // 2 :]), out)
    return out


def turned(seen):
    rows = seen.T
    half, quarter = rows.shape[0] // 2, rows.shape[0] // 4
    return jnp.concatenate(
        [rows[:quarter], rows[half : half + quarter], rows[quarter:half], rows[half + quarter :]], axis=1
    )


def kernel(
    n,
    q_hbm,
    k_hbm,
    v_hbm,
    out_ref,
    q_ref,
    kbuf,
    vbuf,
    part,
    stat,
    parts,
    stats,
    done,
    q_sem,
    k_sem,
    v_sem,
    part_send,
    stat_send,
    part_recv,
    stat_recv,
    done_send,
    done_recv,
):
    me = lax.axis_index("sp")
    cores = 2
    chips = n // cores
    chip, core = lax.div(me, cores), lax.rem(me, cores)
    steps, rows = k_hbm.shape[0], k_hbm.shape[1]
    rounds = steps // chips
    heads = q_ref.shape[0] // (steps * cores)
    head = q_ref.shape[1]

    def chip_of(j):
        away = (chips // 2 - lax.div(j + 1, 2)) * (2 * lax.rem(j, 2) - 1)
        return lax.rem(chip + away + chips, chips)

    def block_of(i):
        return lax.div(i, chips) * chips + chip_of(lax.rem(i, chips))

    def k_copy(i):
        slot = lax.rem(i, SLOTS)
        return pltpu.make_async_copy(k_hbm.at[block_of(i)], kbuf.at[slot], k_sem.at[slot])

    def v_copy(i):
        slot = lax.rem(i, SLOTS)
        return pltpu.make_async_copy(v_hbm.at[block_of(i)], vbuf.at[slot], v_sem.at[slot])

    def send(i, other):
        r, j = lax.div(i, chips), lax.rem(i, chips)
        to = lax.rem(core + other, cores)
        slot = j * cores + 1 - other
        device = {"sp": chip_of(j) * cores + to}
        pltpu.make_async_remote_copy(
            part.at[i, to],
            parts.at[r, slot],
            part_send,
            part_recv.at[r],
            device_id=device,
            device_id_type=MESH,
        ).start()
        pltpu.make_async_remote_copy(
            stat.at[i, to],
            stats.at[r, slot],
            stat_send,
            stat_recv.at[r],
            device_id=device,
            device_id_type=MESH,
        ).start()

    def score(i, j):
        q = q_ref[pl.ds(pl.multiple_of((block_of(i) * cores + j) * heads, heads), heads), :]
        size = rows // cores
        keys = kbuf.at[lax.rem(i, SLOTS), j * size : (j + 1) * size]
        weights, total, high = weights_of(scores_of(q, keys, head))
        stat[i, j] = jnp.concatenate([total, high], axis=0)
        return weights

    def see(i, j, weights):
        size = rows // cores
        values = vbuf.at[lax.rem(i, SLOTS), j * size : (j + 1) * size]
        part[i, j] = seen_of(weights, values, head).astype(BF16)

    def wait_for(ref, sem):
        pltpu.make_async_copy(ref, ref, sem).wait()

    def finish(r):
        own = n - 1
        parts[r, own] = part[r * chips + chips - 1, core]
        stats[r, own] = stat[r * chips + chips - 1, core]
        wait_for(stats.at[r, : n - 1], stat_recv.at[r])
        highs = [stats[r, t][1:2] for t in range(n)]
        high = functools.reduce(jnp.maximum, highs)
        scales = [jnp.exp(x - high) for x in highs]
        total = functools.reduce(jnp.add, [stats[r, t][0:1] * scales[t] for t in range(n)])
        wait_for(parts.at[r, : n - 1], part_recv.at[r])
        seen = functools.reduce(jnp.add, [parts[r, t].astype(F32) * scales[t] for t in range(n)])
        done[r * n + me] = turned(seen / total).astype(BF16)
        for j in range(chips):
            for other in (1, 0):
                if j == chips - 1 and other == 0:
                    continue
                pltpu.make_async_remote_copy(
                    done.at[r * n + me],
                    done.at[r * n + me],
                    done_send,
                    done_recv.at[r],
                    device_id={"sp": chip_of(j) * cores + lax.rem(core + other, cores)},
                    device_id_type=MESH,
                ).start()

    q_copy = pltpu.make_async_copy(q_hbm, q_ref, q_sem)
    q_copy.start()
    for i in range(SLOTS):
        k_copy(i).start()
        if i < SLOTS - 1:
            v_copy(i).start()
    barrier = pltpu.get_barrier_semaphore()
    for away in range(1, n):
        pl.semaphore_signal(barrier, inc=1, device_id={"sp": lax.rem(me + away, n)}, device_id_type=MESH)

    q_copy.wait()
    k_copy(0).wait()
    weights = tuple(score(0, j) for j in range(cores))
    pl.semaphore_wait(barrier, n - 1)

    def step(i, weights):
        k_copy(i + 1).wait()
        v_copy(i).wait()

        @pl.when(i + SLOTS < steps)
        def _():
            k_copy(i + SLOTS).start()

        @pl.when(i + SLOTS - 1 < steps)
        def _():
            v_copy(i + SLOTS - 1).start()

        @pl.when(i > 0)
        def _():
            send(i - 1, 1)

        @pl.when(lax.rem(i, chips) > 0)
        def _():
            send(i - 1, 0)

        later = []
        for j in range(cores):
            later.append(score(i + 1, j))
            see(i, j, weights[j])
        return tuple(later)

    first = 0
    for r in range(rounds - 1):
        until = (r + 1) * chips + EARLY
        weights = lax.fori_loop(first, until, step, weights)
        finish(r)
        first = until
    weights = lax.fori_loop(first, steps - 1, step, weights)
    last = steps - 1
    v_copy(last).wait()
    send(last - 1, 1)
    send(last - 1, 0)
    for j in range(cores):
        see(last, j, weights[j])
    send(last, 1)
    finish(rounds - 1)
    wait_for(parts.at[:, : n - 1], part_send)
    wait_for(stats.at[:, : n - 1], stat_send)
    for r in range(rounds):
        wait_for(done.at[: n - 1], done_send)
    for r in range(rounds):
        wait_for(done.at[: n - 1], done_recv.at[r])
    out_ref[...] = done[...]


def solution(mesh):
    n = mesh.shape["sp"]

    def step(q, k, v):
        sequences, tokens, heads, head = k.shape
        steps = sequences // 2
        keys, values = (jnp.transpose(x, (0, 2, 3, 1)).reshape(steps, 2 * heads * head, tokens) for x in (k, v))
        half = head // 2
        rounds = sequences // n
        out = pl.pallas_call(
            functools.partial(kernel, n),
            out_shape=jax.ShapeDtypeStruct((sequences, heads // 2, 2 * head), BF16),
            in_specs=[pl.BlockSpec(memory_space=pl.ANY)] * 3,
            out_specs=pl.BlockSpec(memory_space=pltpu.VMEM),
            scratch_shapes=[
                pltpu.VMEM((sequences * heads, head), BF16),
                pltpu.VMEM((SLOTS, 2 * heads * head, tokens), BF16),
                pltpu.VMEM((SLOTS, 2 * heads * head, tokens), BF16),
                pltpu.VMEM((steps, 2, half, 2 * heads), BF16),
                pltpu.VMEM((steps, 2, 2, 2 * heads), F32),
                pltpu.VMEM((rounds, n, half, 2 * heads), BF16),
                pltpu.VMEM((rounds, n, 2, 2 * heads), F32),
                pltpu.VMEM((sequences, heads // 2, 2 * head), BF16),
                pltpu.SemaphoreType.DMA(()),
                pltpu.SemaphoreType.DMA((SLOTS,)),
                pltpu.SemaphoreType.DMA((SLOTS,)),
                pltpu.SemaphoreType.DMA(()),
                pltpu.SemaphoreType.DMA(()),
                pltpu.SemaphoreType.DMA((rounds,)),
                pltpu.SemaphoreType.DMA((rounds,)),
                pltpu.SemaphoreType.DMA(()),
                pltpu.SemaphoreType.DMA((rounds,)),
            ],
            compiler_params=pltpu.CompilerParams(collective_id=0, has_side_effects=True),
        )(q.reshape(sequences * heads, head), keys, values)
        return jnp.concatenate([out[..., :head], out[..., head:]], axis=1)

    return jax.shard_map(
        step,
        mesh=mesh,
        in_specs=(P("dp", None, None), P("dp", "sp", None, None), P("dp", "sp", None, None)),
        out_specs=P("dp", None, None),
        check_vma=False,
    )
```

```python
import functools

import jax
import jax.numpy as jnp
from jax import lax
from jax.experimental import pallas as pl
from jax.experimental.pallas import tpu as pltpu
from jax.sharding import PartitionSpec as P

MESH = pl.DeviceIdType.MESH
F32, BF16 = jnp.float32, jnp.bfloat16
SLOTS = 4
EARLY = 3
ROWS = 16


def iota(shape, dim):
    return lax.broadcasted_iota(jnp.int32, shape, dim)


def scores_of(q, keys, head):
    heads = q.shape[0]
    per = 128 // head
    out = []
    for first in range(0, heads, ROWS):
        rows = q[first : first + ROWS]
        wide = jnp.concatenate([rows] * per, axis=1)
        blocks = [
            jnp.where(iota((ROWS, 128), 0) == iota((ROWS, 128), 1) // head + per * j, wide, jnp.zeros_like(wide))
            for j in range(ROWS // per)
        ]
        out.append(
            jnp.dot(
                jnp.concatenate(blocks, axis=1),
                keys[first * head : (first + ROWS) * head],
                preferred_element_type=F32,
            )
        )
    return jnp.concatenate(out, axis=0) * head**-0.5


def row_of(column, heads):
    own = iota((heads, 128), 1) % heads == iota((heads, 128), 0)
    return jnp.sum(jnp.where(own, column, 0.0), axis=0, keepdims=True)


def weights_of(scores):
    heads, tokens = scores.shape
    high = jnp.max(scores, axis=1, keepdims=True)
    weights = jnp.exp(scores - high)
    total = jnp.sum(weights, axis=1, keepdims=True)
    wide = lambda x: jnp.broadcast_to(x, (heads, 128))
    return weights.astype(BF16), row_of(wide(total), heads), row_of(wide(high), heads)


def seen_of(weights, values, head):
    heads, tokens = weights.shape
    half = heads // 2
    nothing = jnp.zeros((half, tokens), BF16)
    lower = jnp.concatenate([weights[:half], nothing] * (128 // heads), axis=0)
    upper = jnp.concatenate([nothing, weights[half:]] * (128 // heads), axis=0)
    both = jnp.concatenate([values[: half * head], values[half * head :]], axis=1)
    products = lax.dot_general(
        both, jnp.concatenate([lower, upper], axis=1), (((1,), (1,)), ((), ())), preferred_element_type=F32
    )
    lane = iota((head // 2, 128), 1)
    out = jnp.zeros((head // 2, 128), F32)
    for h in range(half):
        mine = products[h * head : (h + 1) * head]
        out = jnp.where(lane % half == h, jnp.where(lane < heads, mine[: head // 2], mine[head // 2 :]), out)
    return out


def turned(seen):
    rows = seen.T
    half, quarter = rows.shape[0] // 2, rows.shape[0] // 4
    return jnp.concatenate(
        [rows[:quarter], rows[half : half + quarter], rows[quarter:half], rows[half + quarter :]], axis=1
    )


def kernel(
    n,
    q_hbm,
    k_hbm,
    v_hbm,
    out_ref,
    q_ref,
    kbuf,
    vbuf,
    part,
    stat,
    parts,
    stats,
    done,
    q_sem,
    k_sem,
    v_sem,
    part_send,
    stat_send,
    part_recv,
    stat_recv,
    done_send,
    done_recv,
    near_recv,
    last_sem,
):
    me = lax.axis_index("sp")
    cores = 2
    chips = n // cores
    chip, core = lax.div(me, cores), lax.rem(me, cores)
    steps, rows = k_hbm.shape[0], k_hbm.shape[1]
    rounds = steps // chips
    last = steps - 1
    heads = q_ref.shape[0] // (steps * cores)
    head = q_ref.shape[1]

    def chip_of(j):
        away = (chips // 2 - lax.div(j + 1, 2)) * (2 * lax.rem(j, 2) - 1)
        return lax.rem(chip + away + chips, chips)

    def block_of(i):
        return lax.div(i, chips) * chips + chip_of(lax.rem(i, chips))

    def k_copy(i):
        slot = lax.rem(i, SLOTS)
        return pltpu.make_async_copy(k_hbm.at[block_of(i)], kbuf.at[slot], k_sem.at[slot])

    def v_copy(i):
        slot = lax.rem(i, SLOTS)
        return pltpu.make_async_copy(v_hbm.at[block_of(i)], vbuf.at[slot], v_sem.at[slot])

    def rows_of(other):
        size = rows // cores
        return pl.ds(pl.multiple_of(lax.rem(core + other, cores) * size, size), size)

    def last_copy(other):
        return pltpu.make_async_copy(
            v_hbm.at[block_of(last), rows_of(other)], vbuf.at[last % SLOTS, rows_of(other)], last_sem.at[other]
        )

    def send(i, other):
        r, j = lax.div(i, chips), lax.rem(i, chips)
        to = lax.rem(core + other, cores)
        slot = j * cores + 1 - other
        device = {"sp": chip_of(j) * cores + to}
        pltpu.make_async_remote_copy(
            part.at[i, to],
            parts.at[r, slot],
            part_send,
            part_recv.at[r],
            device_id=device,
            device_id_type=MESH,
        ).start()
        pltpu.make_async_remote_copy(
            stat.at[i, to],
            stats.at[r, slot],
            stat_send,
            stat_recv.at[r],
            device_id=device,
            device_id_type=MESH,
        ).start()

    def score(i, j):
        q = q_ref[pl.ds(pl.multiple_of((block_of(i) * cores + j) * heads, heads), heads), :]
        size = rows // cores
        keys = kbuf.at[lax.rem(i, SLOTS), j * size : (j + 1) * size]
        weights, total, high = weights_of(scores_of(q, keys, head))
        stat[i, j] = jnp.concatenate([total, high], axis=0)
        return weights

    def see(i, j, weights):
        size = rows // cores
        values = vbuf.at[lax.rem(i, SLOTS), j * size : (j + 1) * size]
        part[i, j] = seen_of(weights, values, head).astype(BF16)

    def wait_for(ref, sem):
        pltpu.make_async_copy(ref, ref, sem).wait()

    def finish(r):
        own = n - 1
        parts[r, own] = part[r * chips + chips - 1, core]
        stats[r, own] = stat[r * chips + chips - 1, core]
        wait_for(stats.at[r, : n - 1], stat_recv.at[r])
        highs = [stats[r, t][1:2] for t in range(n)]
        high = functools.reduce(jnp.maximum, highs)
        scales = [jnp.exp(x - high) for x in highs]
        total = functools.reduce(jnp.add, [stats[r, t][0:1] * scales[t] for t in range(n)])
        wait_for(parts.at[r, : n - 1], part_recv.at[r])
        seen = functools.reduce(jnp.add, [parts[r, t].astype(F32) * scales[t] for t in range(n)])
        done[r * n + me] = turned(seen / total).astype(BF16)
        return r * n + me

    def share(which, device, sem):
        pltpu.make_async_remote_copy(
            done.at[which], done.at[which], done_send, sem, device_id={"sp": device}, device_id_type=MESH
        ).start()

    def gather(r):
        for j in range(chips):
            for other in (1, 0):
                if j < chips - 1 or other:
                    share(r * n + me, chip_of(j) * cores + lax.rem(core + other, cores), done_recv.at[r])

    def relay(r):
        partner = chip * cores + lax.rem(core + 1, cores)
        for j in range(chips - 1):
            share(r * n + me, chip_of(j) * cores + core, near_recv.at[j])
            if j == 0:
                share(r * n + me, chip_of(j) * cores + lax.rem(core + 1, cores), done_recv.at[r])
        share(r * n + me, partner, done_recv.at[r])
        for j in reversed(range(chips - 1)):
            wait_for(done.at[0], near_recv.at[j])
            if j > 0:
                away = (chips // 2 - (j + 1) // 2) * (2 * (j % 2) - 1)
                share(r * n + lax.rem(chip - away + chips, chips) * cores + core, partner, done_recv.at[r])

    q_copy = pltpu.make_async_copy(q_hbm, q_ref, q_sem)
    q_copy.start()
    for i in range(SLOTS):
        k_copy(i).start()
        if i < SLOTS - 1:
            v_copy(i).start()
    barrier = pltpu.get_barrier_semaphore()
    for away in range(1, n):
        pl.semaphore_signal(barrier, inc=1, device_id={"sp": lax.rem(me + away, n)}, device_id_type=MESH)

    q_copy.wait()
    k_copy(0).wait()
    weights = tuple(score(0, j) for j in range(cores))
    pl.semaphore_wait(barrier, n - 1)

    def step(i, weights):
        k_copy(i + 1).wait()
        v_copy(i).wait()

        @pl.when(i + SLOTS < steps)
        def _():
            k_copy(i + SLOTS).start()

        @pl.when(i + SLOTS - 1 < last)
        def _():
            v_copy(i + SLOTS - 1).start()

        @pl.when(i + SLOTS - 1 == last)
        def _():
            for other in (1, 0):
                last_copy(other).start()

        @pl.when(i > 0)
        def _():
            send(i - 1, 1)

        @pl.when(lax.rem(i, chips) > 0)
        def _():
            send(i - 1, 0)

        later = []
        for j in range(cores):
            later.append(score(i + 1, j))
            see(i, j, weights[j])
        return tuple(later)

    first = 0
    for r in range(rounds - 1):
        until = (r + 1) * chips + EARLY
        weights = lax.fori_loop(first, until, step, weights)
        finish(r)
        gather(r)
        first = until
    weights = lax.fori_loop(first, last, step, weights)
    for other in (1, 0):
        send(last - 1, other)
    mine = [x.astype(F32) for x in weights]
    for other in (1, 0):
        ours = jnp.where(lax.rem(core + other, cores) == 0, *mine).astype(BF16)
        last_copy(other).wait()
        part[last, lax.rem(core + other, cores)] = seen_of(ours, vbuf.at[last % SLOTS, rows_of(other)], head).astype(BF16)
        if other:
            send(last, other)
    finish(rounds - 1)
    relay(rounds - 1)
    wait_for(parts.at[:, : n - 1], part_send)
    wait_for(stats.at[:, : n - 1], stat_send)
    for r in range(rounds):
        wait_for(done.at[: n - 1], done_send)
    for r in range(rounds - 1):
        wait_for(done.at[: n - 1], done_recv.at[r])
    wait_for(done.at[:chips], done_recv.at[rounds - 1])
    out_ref[...] = done[...]


def unpack(packed_ref, out_ref):
    half, head = packed_ref.shape[1], out_ref.shape[2]
    out_ref[:, :half] = packed_ref[:, :, :head]
    out_ref[:, half:] = packed_ref[:, :, head:]


def solution(mesh):
    n = mesh.shape["sp"]

    def step(q, k, v):
        sequences, tokens, heads, head = k.shape
        steps = sequences // 2
        keys, values = (jnp.transpose(x, (0, 2, 3, 1)).reshape(steps, 2 * heads * head, tokens) for x in (k, v))
        half = head // 2
        rounds = sequences // n
        out = pl.pallas_call(
            functools.partial(kernel, n),
            out_shape=pltpu.VMEM((sequences, heads // 2, 2 * head), BF16),
            in_specs=[pl.BlockSpec(memory_space=pl.ANY)] * 3,
            out_specs=pl.BlockSpec(memory_space=pltpu.VMEM),
            scratch_shapes=[
                pltpu.VMEM((sequences * heads, head), BF16),
                pltpu.VMEM((SLOTS, 2 * heads * head, tokens), BF16),
                pltpu.VMEM((SLOTS, 2 * heads * head, tokens), BF16),
                pltpu.VMEM((steps, 2, half, 2 * heads), BF16),
                pltpu.VMEM((steps, 2, 2, 2 * heads), F32),
                pltpu.VMEM((rounds, n, half, 2 * heads), BF16),
                pltpu.VMEM((rounds, n, 2, 2 * heads), F32),
                pltpu.VMEM((sequences, heads // 2, 2 * head), BF16),
                pltpu.SemaphoreType.DMA(()),
                pltpu.SemaphoreType.DMA((SLOTS,)),
                pltpu.SemaphoreType.DMA((SLOTS,)),
                pltpu.SemaphoreType.DMA(()),
                pltpu.SemaphoreType.DMA(()),
                pltpu.SemaphoreType.DMA((rounds,)),
                pltpu.SemaphoreType.DMA((rounds,)),
                pltpu.SemaphoreType.DMA(()),
                pltpu.SemaphoreType.DMA((rounds,)),
                pltpu.SemaphoreType.DMA((n // 2 - 1,)),
                pltpu.SemaphoreType.DMA((2,)),
            ],
            compiler_params=pltpu.CompilerParams(collective_id=0, has_side_effects=True),
        )(q.reshape(sequences * heads, head), keys, values)
        return pl.pallas_call(
            unpack,
            out_shape=jax.ShapeDtypeStruct(q.shape, BF16),
            in_specs=[pl.BlockSpec(memory_space=pltpu.VMEM)],
            out_specs=pl.BlockSpec(memory_space=pltpu.VMEM),
        )(pltpu.with_memory_space_constraint(out, pltpu.VMEM))

    return jax.shard_map(
        step,
        mesh=mesh,
        in_specs=(P("dp", None, None), P("dp", "sp", None, None), P("dp", "sp", None, None)),
        out_specs=P("dp", None, None),
        check_vma=False,
    )
```

```python
import functools

import jax
import jax.numpy as jnp
from jax import lax
from jax.experimental import pallas as pl
from jax.experimental.pallas import tpu as pltpu
from jax.sharding import PartitionSpec as P

MESH = pl.DeviceIdType.MESH
F32, BF16 = jnp.float32, jnp.bfloat16
SLOTS = 4
QUIET = 4
EARLY = 3
ROWS = 16


def iota(shape, dim):
    return lax.broadcasted_iota(jnp.int32, shape, dim)


def scores_of(q, keys, head):
    heads = q.shape[0]
    per = 128 // head
    out = []
    for first in range(0, heads, ROWS):
        rows = q[first : first + ROWS]
        wide = jnp.concatenate([rows] * per, axis=1)
        blocks = [
            jnp.where(iota((ROWS, 128), 0) == iota((ROWS, 128), 1) // head + per * j, wide, jnp.zeros_like(wide))
            for j in range(ROWS // per)
        ]
        out.append(
            jnp.dot(
                jnp.concatenate(blocks, axis=1),
                keys[first * head : (first + ROWS) * head],
                preferred_element_type=F32,
            )
        )
    return jnp.concatenate(out, axis=0) * head**-0.5


def row_of(column, heads):
    own = iota((heads, 128), 1) % heads == iota((heads, 128), 0)
    return jnp.sum(jnp.where(own, column, 0.0), axis=0, keepdims=True)


def weights_of(scores):
    heads, tokens = scores.shape
    high = jnp.max(scores, axis=1, keepdims=True)
    weights = jnp.exp(scores - high)
    total = jnp.sum(weights, axis=1, keepdims=True)
    wide = lambda x: jnp.broadcast_to(x, (heads, 128))
    return weights.astype(BF16), row_of(wide(total), heads), row_of(wide(high), heads)


def seen_of(weights, values, head):
    heads, tokens = weights.shape
    half = heads // 2
    nothing = jnp.zeros((half, tokens), BF16)
    lower = jnp.concatenate([weights[:half], nothing] * (128 // heads), axis=0)
    upper = jnp.concatenate([nothing, weights[half:]] * (128 // heads), axis=0)
    both = jnp.concatenate([values[: half * head], values[half * head :]], axis=1)
    products = lax.dot_general(
        both, jnp.concatenate([lower, upper], axis=1), (((1,), (1,)), ((), ())), preferred_element_type=F32
    )
    lane = iota((head // 2, 128), 1)
    out = jnp.zeros((head // 2, 128), F32)
    for h in range(half):
        mine = products[h * head : (h + 1) * head]
        out = jnp.where(lane % half == h, jnp.where(lane < heads, mine[: head // 2], mine[head // 2 :]), out)
    return out


def turned(seen):
    rows = seen.T
    half, quarter = rows.shape[0] // 2, rows.shape[0] // 4
    return jnp.concatenate(
        [rows[:quarter], rows[half : half + quarter], rows[quarter:half], rows[half + quarter :]], axis=1
    )


def kernel(
    n,
    q_hbm,
    k_hbm,
    v_hbm,
    out_ref,
    q_ref,
    kbuf,
    vbuf,
    part,
    stat,
    parts,
    stats,
    done,
    q_sem,
    k_sem,
    v_sem,
    part_send,
    stat_send,
    part_recv,
    stat_recv,
    done_send,
    done_recv,
    near_recv,
    last_sem,
):
    me = lax.axis_index("sp")
    cores = 2
    chips = n // cores
    chip, core = lax.div(me, cores), lax.rem(me, cores)
    steps, rows = k_hbm.shape[0], k_hbm.shape[1]
    rounds = steps // chips
    last = steps - 1
    heads = q_ref.shape[0] // (steps * cores)
    head = q_ref.shape[1]

    def chip_of(j):
        away = (chips // 2 - lax.div(j + 1, 2)) * (2 * lax.rem(j, 2) - 1)
        return lax.rem(chip + away + chips, chips)

    def block_of(i):
        return lax.div(i, chips) * chips + chip_of(lax.rem(i, chips))

    def k_copy(i):
        slot = lax.rem(i, SLOTS)
        return pltpu.make_async_copy(k_hbm.at[block_of(i)], kbuf.at[slot], k_sem.at[slot])

    def v_copy(i):
        slot = lax.rem(i, SLOTS)
        return pltpu.make_async_copy(v_hbm.at[block_of(i)], vbuf.at[slot], v_sem.at[slot])

    def rows_of(other):
        size = rows // cores
        return pl.ds(pl.multiple_of(lax.rem(core + other, cores) * size, size), size)

    def last_copy(other):
        return pltpu.make_async_copy(
            v_hbm.at[block_of(last), rows_of(other)], vbuf.at[last % SLOTS, rows_of(other)], last_sem.at[other]
        )

    def send(i, other):
        r, j = lax.div(i, chips), lax.rem(i, chips)
        to = lax.rem(core + other, cores)
        slot = j * cores + 1 - other
        device = {"sp": chip_of(j) * cores + to}
        pltpu.make_async_remote_copy(
            part.at[i, to],
            parts.at[r, slot],
            part_send,
            part_recv.at[r],
            device_id=device,
            device_id_type=MESH,
        ).start()
        pltpu.make_async_remote_copy(
            stat.at[i, to],
            stats.at[r, slot],
            stat_send,
            stat_recv.at[r],
            device_id=device,
            device_id_type=MESH,
        ).start()

    def score(i, j):
        q = q_ref[pl.ds(pl.multiple_of((block_of(i) * cores + j) * heads, heads), heads), :]
        size = rows // cores
        keys = kbuf.at[lax.rem(i, SLOTS), j * size : (j + 1) * size]
        weights, total, high = weights_of(scores_of(q, keys, head))
        stat[i, j] = jnp.concatenate([total, high], axis=0)
        return weights

    def see(i, j, weights):
        size = rows // cores
        values = vbuf.at[lax.rem(i, SLOTS), j * size : (j + 1) * size]
        part[i, j] = seen_of(weights, values, head).astype(BF16)

    def wait_for(ref, sem):
        pltpu.make_async_copy(ref, ref, sem).wait()

    def finish(r):
        own = n - 1
        parts[r, own] = part[r * chips + chips - 1, core]
        stats[r, own] = stat[r * chips + chips - 1, core]
        wait_for(stats.at[r, : n - 1], stat_recv.at[r])
        highs = [stats[r, t][1:2] for t in range(n)]
        high = functools.reduce(jnp.maximum, highs)
        scales = [jnp.exp(x - high) for x in highs]
        total = functools.reduce(jnp.add, [stats[r, t][0:1] * scales[t] for t in range(n)])
        wait_for(parts.at[r, : n - 1], part_recv.at[r])
        seen = functools.reduce(jnp.add, [parts[r, t].astype(F32) * scales[t] for t in range(n)])
        done[r * n + me] = turned(seen / total).astype(BF16)
        return r * n + me

    def share(which, device, sem):
        pltpu.make_async_remote_copy(
            done.at[which], done.at[which], done_send, sem, device_id={"sp": device}, device_id_type=MESH
        ).start()

    def gather(r):
        for j in range(chips):
            for other in (1, 0):
                if j < chips - 1 or other:
                    share(r * n + me, chip_of(j) * cores + lax.rem(core + other, cores), done_recv.at[r])

    def relay(r):
        partner = chip * cores + lax.rem(core + 1, cores)
        for j in range(chips - 1):
            share(r * n + me, chip_of(j) * cores + core, near_recv.at[j])
            if j == 0:
                share(r * n + me, chip_of(j) * cores + lax.rem(core + 1, cores), done_recv.at[r])
        share(r * n + me, partner, done_recv.at[r])
        for j in reversed(range(chips - 1)):
            wait_for(done.at[0], near_recv.at[j])
            if j > 0:
                away = (chips // 2 - (j + 1) // 2) * (2 * (j % 2) - 1)
                share(r * n + lax.rem(chip - away + chips, chips) * cores + core, partner, done_recv.at[r])

    q_copy = pltpu.make_async_copy(q_hbm, q_ref, q_sem)
    q_copy.start()
    for i in range(SLOTS):
        k_copy(i).start()
        if i < SLOTS - 1:
            v_copy(i).start()
    barrier = pltpu.get_barrier_semaphore()
    for away in range(1, n):
        pl.semaphore_signal(barrier, inc=1, device_id={"sp": lax.rem(me + away, n)}, device_id_type=MESH)

    q_copy.wait()
    k_copy(0).wait()
    weights = tuple(score(0, j) for j in range(cores))

    def step(first, i, weights):
        k_copy(i + 1).wait()
        v_copy(i).wait()

        @pl.when(i + SLOTS < steps)
        def _():
            k_copy(i + SLOTS).start()

        @pl.when(i + SLOTS - 1 < last)
        def _():
            v_copy(i + SLOTS - 1).start()

        @pl.when(i + SLOTS - 1 == last)
        def _():
            for other in (1, 0):
                last_copy(other).start()

        if first:

            @pl.when(i > first)
            def _():
                for other in (1, 0):
                    send(i - 1, other)

        later = []
        for j in range(cores):
            later.append(score(i + 1, j))
            see(i, j, weights[j])
        return tuple(later)

    weights = lax.fori_loop(0, QUIET, functools.partial(step, None), weights)
    pl.semaphore_wait(barrier, n - 1)

    def send_both(i, _):
        for other in (1, 0):
            send(i, other)

    lax.fori_loop(0, QUIET, send_both, None)
    first = QUIET
    for r in range(rounds - 1):
        middle, until = (r + 1) * chips, (r + 1) * chips + EARLY
        weights = lax.fori_loop(first, middle, functools.partial(step, first), weights)
        send(middle - 1, 1)
        weights = lax.fori_loop(middle, until, functools.partial(step, middle), weights)
        send_both(until - 1, None)
        finish(r)
        gather(r)
        first = until
    weights = lax.fori_loop(first, last, functools.partial(step, first), weights)
    for other in (1, 0):
        send(last - 1, other)
    mine = [x.astype(F32) for x in weights]
    for other in (1, 0):
        ours = jnp.where(lax.rem(core + other, cores) == 0, *mine).astype(BF16)
        last_copy(other).wait()
        part[last, lax.rem(core + other, cores)] = seen_of(ours, vbuf.at[last % SLOTS, rows_of(other)], head).astype(BF16)
        if other:
            send(last, other)
    finish(rounds - 1)
    relay(rounds - 1)
    wait_for(parts.at[:, : n - 1], part_send)
    wait_for(stats.at[:, : n - 1], stat_send)
    for r in range(rounds):
        wait_for(done.at[: n - 1], done_send)
    for r in range(rounds - 1):
        wait_for(done.at[: n - 1], done_recv.at[r])
    wait_for(done.at[:chips], done_recv.at[rounds - 1])
    out_ref[...] = done[...]


def unpack(packed_ref, out_ref):
    half, head = packed_ref.shape[1], out_ref.shape[2]
    out_ref[:, :half] = packed_ref[:, :, :head]
    out_ref[:, half:] = packed_ref[:, :, head:]


def solution(mesh):
    n = mesh.shape["sp"]

    def step(q, k, v):
        sequences, tokens, heads, head = k.shape
        steps = sequences // 2
        keys, values = (jnp.transpose(x, (0, 2, 3, 1)).reshape(steps, 2 * heads * head, tokens) for x in (k, v))
        half = head // 2
        rounds = sequences // n
        out = pl.pallas_call(
            functools.partial(kernel, n),
            out_shape=pltpu.VMEM((sequences, heads // 2, 2 * head), BF16),
            in_specs=[pl.BlockSpec(memory_space=pl.ANY)] * 3,
            out_specs=pl.BlockSpec(memory_space=pltpu.VMEM),
            scratch_shapes=[
                pltpu.VMEM((sequences * heads, head), BF16),
                pltpu.VMEM((SLOTS, 2 * heads * head, tokens), BF16),
                pltpu.VMEM((SLOTS, 2 * heads * head, tokens), BF16),
                pltpu.VMEM((steps, 2, half, 2 * heads), BF16),
                pltpu.VMEM((steps, 2, 2, 2 * heads), F32),
                pltpu.VMEM((rounds, n, half, 2 * heads), BF16),
                pltpu.VMEM((rounds, n, 2, 2 * heads), F32),
                pltpu.VMEM((sequences, heads // 2, 2 * head), BF16),
                pltpu.SemaphoreType.DMA(()),
                pltpu.SemaphoreType.DMA((SLOTS,)),
                pltpu.SemaphoreType.DMA((SLOTS,)),
                pltpu.SemaphoreType.DMA(()),
                pltpu.SemaphoreType.DMA(()),
                pltpu.SemaphoreType.DMA((rounds,)),
                pltpu.SemaphoreType.DMA((rounds,)),
                pltpu.SemaphoreType.DMA(()),
                pltpu.SemaphoreType.DMA((rounds,)),
                pltpu.SemaphoreType.DMA((n // 2 - 1,)),
                pltpu.SemaphoreType.DMA((2,)),
            ],
            compiler_params=pltpu.CompilerParams(collective_id=0, has_side_effects=True),
        )(q.reshape(sequences * heads, head), keys, values)
        return pl.pallas_call(
            unpack,
            out_shape=jax.ShapeDtypeStruct(q.shape, BF16),
            in_specs=[pl.BlockSpec(memory_space=pltpu.VMEM)],
            out_specs=pl.BlockSpec(memory_space=pltpu.VMEM),
        )(pltpu.with_memory_space_constraint(out, pltpu.VMEM))

    return jax.shard_map(
        step,
        mesh=mesh,
        in_specs=(P("dp", None, None), P("dp", "sp", None, None), P("dp", "sp", None, None)),
        out_specs=P("dp", None, None),
        check_vma=False,
    )
```

```python
import functools

import jax
import jax.numpy as jnp
from jax import lax
from jax.experimental import pallas as pl
from jax.experimental.pallas import tpu as pltpu
from jax.sharding import PartitionSpec as P

MESH = pl.DeviceIdType.MESH
F32, BF16 = jnp.float32, jnp.bfloat16
SLOTS = 4
QUIET = 4
EARLY = 3
ROWS = 16


def iota(shape, dim):
    return lax.broadcasted_iota(jnp.int32, shape, dim)


def scores_of(q, keys, head):
    heads = q.shape[0]
    per = 128 // head
    out = []
    for first in range(0, heads, ROWS):
        rows = q[first : first + ROWS]
        wide = jnp.concatenate([rows] * per, axis=1)
        blocks = [
            jnp.where(iota((ROWS, 128), 0) == iota((ROWS, 128), 1) // head + per * j, wide, jnp.zeros_like(wide))
            for j in range(ROWS // per)
        ]
        out.append(
            jnp.dot(
                jnp.concatenate(blocks, axis=1),
                keys[first * head : (first + ROWS) * head],
                preferred_element_type=F32,
            )
        )
    return jnp.concatenate(out, axis=0) * head**-0.5


def row_of(column, heads):
    own = iota((heads, 128), 1) % heads == iota((heads, 128), 0)
    return jnp.sum(jnp.where(own, column, 0.0), axis=0, keepdims=True)


def weights_of(scores):
    heads, tokens = scores.shape
    high = jnp.max(scores, axis=1, keepdims=True)
    weights = jnp.exp(scores - high)
    total = jnp.sum(weights, axis=1, keepdims=True)
    wide = lambda x: jnp.broadcast_to(x, (heads, 128))
    return weights.astype(BF16), row_of(wide(total), heads), row_of(wide(high), heads)


def seen_of(weights, values, head):
    heads, tokens = weights.shape
    half = heads // 2
    nothing = jnp.zeros((half, tokens), BF16)
    lower = jnp.concatenate([weights[:half], nothing] * (128 // heads), axis=0)
    upper = jnp.concatenate([nothing, weights[half:]] * (128 // heads), axis=0)
    both = jnp.concatenate([values[: half * head], values[half * head :]], axis=1)
    products = lax.dot_general(
        both, jnp.concatenate([lower, upper], axis=1), (((1,), (1,)), ((), ())), preferred_element_type=F32
    )
    lane = iota((head // 2, 128), 1)
    out = jnp.zeros((head // 2, 128), F32)
    for h in range(half):
        mine = products[h * head : (h + 1) * head]
        out = jnp.where(lane % half == h, jnp.where(lane < heads, mine[: head // 2], mine[head // 2 :]), out)
    return out


def turned(seen):
    rows = seen.T
    half, quarter = rows.shape[0] // 2, rows.shape[0] // 4
    return jnp.concatenate(
        [rows[:quarter], rows[half : half + quarter], rows[quarter:half], rows[half + quarter :]], axis=1
    )


def kernel(
    n,
    q_hbm,
    k_hbm,
    v_hbm,
    out_ref,
    q_ref,
    kbuf,
    vbuf,
    part,
    stat,
    parts,
    stats,
    done,
    q_sem,
    k_sem,
    v_sem,
    part_send,
    stat_send,
    part_recv,
    stat_recv,
    done_send,
    done_recv,
    near_recv,
    last_sem,
):
    me = lax.axis_index("sp")
    cores = 2
    chips = n // cores
    chip, core = lax.div(me, cores), lax.rem(me, cores)
    steps, rows = k_hbm.shape[0], k_hbm.shape[1]
    rounds = steps // chips
    last = steps - 1
    heads = q_ref.shape[0] // (steps * cores)
    head = q_ref.shape[1]

    def chip_of(j):
        away = (chips // 2 - lax.div(j + 1, 2)) * (2 * lax.rem(j, 2) - 1)
        return lax.rem(chip + away + chips, chips)

    def block_of(i):
        return lax.div(i, chips) * chips + chip_of(lax.rem(i, chips))

    def k_copy(i, block=0):
        slot = lax.rem(i, SLOTS)
        return pltpu.make_async_copy(k_hbm.at[block], kbuf.at[slot], k_sem.at[slot])

    def v_copy(i, block=0):
        slot = lax.rem(i, SLOTS)
        return pltpu.make_async_copy(v_hbm.at[block], vbuf.at[slot], v_sem.at[slot])

    def first_copy(j):
        size = rows // cores
        own = pl.ds(j * size, size)
        return pltpu.make_async_copy(k_hbm.at[block_of(0), own], kbuf.at[0, own], last_sem.at[j])

    def rows_of(other):
        size = rows // cores
        return pl.ds(pl.multiple_of(lax.rem(core + other, cores) * size, size), size)

    def last_copy(other):
        return pltpu.make_async_copy(
            v_hbm.at[block_of(last), rows_of(other)], vbuf.at[last % SLOTS, rows_of(other)], last_sem.at[other]
        )

    def send(i, other, r, owner):
        j = i - r * chips
        to = lax.rem(core + other, cores)
        slot = j * cores + 1 - other
        device = {"sp": owner * cores + to}
        pltpu.make_async_remote_copy(
            part.at[i, to],
            parts.at[r, slot],
            part_send,
            part_recv.at[r],
            device_id=device,
            device_id_type=MESH,
        ).start()
        pltpu.make_async_remote_copy(
            stat.at[i, to],
            stats.at[r, slot],
            stat_send,
            stat_recv.at[r],
            device_id=device,
            device_id_type=MESH,
        ).start()

    def score(i, j, block):
        q = q_ref[pl.ds(pl.multiple_of((block * cores + j) * heads, heads), heads), :]
        size = rows // cores
        keys = kbuf.at[lax.rem(i, SLOTS), j * size : (j + 1) * size]
        weights, total, high = weights_of(scores_of(q, keys, head))
        stat[i, j] = jnp.concatenate([total, high], axis=0)
        return weights

    def see(i, j, weights):
        size = rows // cores
        values = vbuf.at[lax.rem(i, SLOTS), j * size : (j + 1) * size]
        part[i, j] = seen_of(weights, values, head).astype(BF16)

    def wait_for(ref, sem):
        pltpu.make_async_copy(ref, ref, sem).wait()

    def finish(r):
        own = n - 1
        parts[r, own] = part[r * chips + chips - 1, core]
        stats[r, own] = stat[r * chips + chips - 1, core]
        wait_for(stats.at[r, : n - 1], stat_recv.at[r])
        highs = [stats[r, t][1:2] for t in range(n)]
        high = functools.reduce(jnp.maximum, highs)
        scales = [jnp.exp(x - high) for x in highs]
        total = functools.reduce(jnp.add, [stats[r, t][0:1] * scales[t] for t in range(n)])
        wait_for(parts.at[r, : n - 1], part_recv.at[r])
        seen = functools.reduce(jnp.add, [parts[r, t].astype(F32) * scales[t] for t in range(n)])
        done[r * n + me] = turned(seen / total).astype(BF16)
        return r * n + me

    def share(which, device, sem):
        pltpu.make_async_remote_copy(
            done.at[which], done.at[which], done_send, sem, device_id={"sp": device}, device_id_type=MESH
        ).start()

    def gather(r):
        for j in range(chips):
            for other in (1, 0):
                if j < chips - 1 or other:
                    share(r * n + me, chip_of(j) * cores + lax.rem(core + other, cores), done_recv.at[r])

    def relay(r):
        partner = chip * cores + lax.rem(core + 1, cores)
        for j in range(chips - 1):
            share(r * n + me, chip_of(j) * cores + core, near_recv.at[j])
            if j == 0:
                share(r * n + me, chip_of(j) * cores + lax.rem(core + 1, cores), done_recv.at[r])
        share(r * n + me, partner, done_recv.at[r])
        for j in reversed(range(chips - 1)):
            wait_for(done.at[0], near_recv.at[j])
            if j > 0:
                away = (chips // 2 - (j + 1) // 2) * (2 * (j % 2) - 1)
                share(r * n + lax.rem(chip - away + chips, chips) * cores + core, partner, done_recv.at[r])

    q_copy = pltpu.make_async_copy(q_hbm, q_ref, q_sem)
    q_copy.start()
    for i in range(SLOTS):
        if i:
            k_copy(i, block_of(i)).start()
        else:
            for j in range(cores):
                first_copy(j).start()
        if i < SLOTS - 1:
            v_copy(i, block_of(i)).start()
    barrier = pltpu.get_barrier_semaphore()
    for away in range(1, n):
        pl.semaphore_signal(barrier, inc=1, device_id={"sp": lax.rem(me + away, n)}, device_id_type=MESH)

    q_copy.wait()
    start = block_of(0)
    weights = []
    for j in range(cores):
        first_copy(j).wait()
        weights.append(score(0, j, start))

    def step(first, i, state):
        blocks, weights = state
        k_copy(i + 1).wait()
        v_copy(i).wait()

        @pl.when(i + SLOTS < steps)
        def _():
            k_copy(i + SLOTS, blocks[-1]).start()

        @pl.when(i + SLOTS - 1 < last)
        def _():
            v_copy(i + SLOTS - 1, blocks[-2]).start()

        @pl.when(i + SLOTS - 1 == last)
        def _():
            for other in (1, 0):
                last_copy(other).start()

        if first:

            @pl.when(i > first)
            def _():
                r = first // chips
                for other in (1, 0):
                    send(i - 1, other, r, blocks[0] - r * chips)

        later = []
        for j in range(cores):
            later.append(score(i + 1, j, blocks[2]))
            see(i, j, weights[j])
        return (*blocks[1:], block_of(lax.rem(i + SLOTS + 1, steps))), tuple(later)

    state = (start, *(block_of(i) for i in range(SLOTS + 1))), tuple(weights)
    state = lax.fori_loop(0, QUIET, functools.partial(step, None), state)
    pl.semaphore_wait(barrier, n - 1)

    def send_both(i, _):
        for other in (1, 0):
            send(i, other, 0, chip_of(i))

    lax.fori_loop(0, QUIET, send_both, None)
    first = QUIET
    for r in range(rounds - 1):
        middle, until = (r + 1) * chips, (r + 1) * chips + EARLY
        state = lax.fori_loop(first, middle, functools.partial(step, first), state)
        send(middle - 1, 1, r, chip)
        state = lax.fori_loop(middle, until, functools.partial(step, middle), state)
        for other in (1, 0):
            send(until - 1, other, r + 1, chip_of(EARLY - 1))
        finish(r)
        gather(r)
        first = until
    _, weights = lax.fori_loop(first, last, functools.partial(step, first), state)
    for other in (1, 0):
        send(last - 1, other, rounds - 1, chip_of(chips - 2))
    mine = [x.astype(F32) for x in weights]
    for other in (1, 0):
        ours = jnp.where(lax.rem(core + other, cores) == 0, *mine).astype(BF16)
        last_copy(other).wait()
        part[last, lax.rem(core + other, cores)] = seen_of(ours, vbuf.at[last % SLOTS, rows_of(other)], head).astype(BF16)
        if other:
            send(last, other, rounds - 1, chip)
    finish(rounds - 1)
    relay(rounds - 1)
    wait_for(parts.at[:, : n - 1], part_send)
    wait_for(stats.at[:, : n - 1], stat_send)
    for r in range(rounds):
        wait_for(done.at[: n - 1], done_send)
    for r in range(rounds - 1):
        wait_for(done.at[: n - 1], done_recv.at[r])
    wait_for(done.at[:chips], done_recv.at[rounds - 1])
    out_ref[...] = done[...]


def unpack(packed_ref, out_ref):
    half, head = packed_ref.shape[1], out_ref.shape[2]
    out_ref[:, :half] = packed_ref[:, :, :head]
    out_ref[:, half:] = packed_ref[:, :, head:]


def solution(mesh):
    n = mesh.shape["sp"]

    def step(q, k, v):
        sequences, tokens, heads, head = k.shape
        steps = sequences // 2
        keys, values = (jnp.transpose(x, (0, 2, 3, 1)).reshape(steps, 2 * heads * head, tokens) for x in (k, v))
        half = head // 2
        rounds = sequences // n
        out = pl.pallas_call(
            functools.partial(kernel, n),
            out_shape=pltpu.VMEM((sequences, heads // 2, 2 * head), BF16),
            in_specs=[pl.BlockSpec(memory_space=pl.ANY)] * 3,
            out_specs=pl.BlockSpec(memory_space=pltpu.VMEM),
            scratch_shapes=[
                pltpu.VMEM((sequences * heads, head), BF16),
                pltpu.VMEM((SLOTS, 2 * heads * head, tokens), BF16),
                pltpu.VMEM((SLOTS, 2 * heads * head, tokens), BF16),
                pltpu.VMEM((steps, 2, half, 2 * heads), BF16),
                pltpu.VMEM((steps, 2, 2, 2 * heads), F32),
                pltpu.VMEM((rounds, n, half, 2 * heads), BF16),
                pltpu.VMEM((rounds, n, 2, 2 * heads), F32),
                pltpu.VMEM((sequences, heads // 2, 2 * head), BF16),
                pltpu.SemaphoreType.DMA(()),
                pltpu.SemaphoreType.DMA((SLOTS,)),
                pltpu.SemaphoreType.DMA((SLOTS,)),
                pltpu.SemaphoreType.DMA(()),
                pltpu.SemaphoreType.DMA(()),
                pltpu.SemaphoreType.DMA((rounds,)),
                pltpu.SemaphoreType.DMA((rounds,)),
                pltpu.SemaphoreType.DMA(()),
                pltpu.SemaphoreType.DMA((rounds,)),
                pltpu.SemaphoreType.DMA((n // 2 - 1,)),
                pltpu.SemaphoreType.DMA((2,)),
            ],
            compiler_params=pltpu.CompilerParams(collective_id=0, has_side_effects=True),
        )(q.reshape(sequences * heads, head), keys, values)
        return pl.pallas_call(
            unpack,
            out_shape=jax.ShapeDtypeStruct(q.shape, BF16),
            in_specs=[pl.BlockSpec(memory_space=pltpu.VMEM)],
            out_specs=pl.BlockSpec(memory_space=pltpu.VMEM),
        )(pltpu.with_memory_space_constraint(out, pltpu.VMEM))

    return jax.shard_map(
        step,
        mesh=mesh,
        in_specs=(P("dp", None, None), P("dp", "sp", None, None), P("dp", "sp", None, None)),
        out_specs=P("dp", None, None),
        check_vma=False,
    )
```

```python
import functools

import jax
import jax.numpy as jnp
from jax import lax
from jax.experimental import pallas as pl
from jax.experimental.pallas import tpu as pltpu
from jax.sharding import PartitionSpec as P

MESH = pl.DeviceIdType.MESH
F32, BF16 = jnp.float32, jnp.bfloat16
SLOTS = 3
QUIET = 4
EARLY = 3
ROWS = 16


def iota(shape, dim):
    return lax.broadcasted_iota(jnp.int32, shape, dim)


def scores_of(q, keys, head):
    heads = q.shape[0]
    per = 128 // head
    out = []
    for first in range(0, heads, ROWS):
        rows = q[first : first + ROWS]
        wide = jnp.concatenate([rows] * per, axis=1)
        blocks = [
            jnp.where(iota((ROWS, 128), 0) == iota((ROWS, 128), 1) // head + per * j, wide, jnp.zeros_like(wide))
            for j in range(ROWS // per)
        ]
        out.append(
            jnp.dot(
                jnp.concatenate(blocks, axis=1),
                keys[first * head : (first + ROWS) * head],
                preferred_element_type=F32,
            )
        )
    return jnp.concatenate(out, axis=0) * head**-0.5


def row_of(column, heads):
    own = iota((heads, 128), 1) % heads == iota((heads, 128), 0)
    return jnp.sum(jnp.where(own, column, 0.0), axis=0, keepdims=True)


def weights_of(scores):
    heads, tokens = scores.shape
    high = jnp.max(scores, axis=1, keepdims=True)
    weights = jnp.exp(scores - high)
    total = jnp.sum(weights, axis=1, keepdims=True)
    wide = lambda x: jnp.broadcast_to(x, (heads, 128))
    return weights.astype(BF16), row_of(wide(total), heads), row_of(wide(high), heads)


def seen_of(weights, values, head):
    heads, tokens = weights.shape
    half = heads // 2
    nothing = jnp.zeros((half, tokens), BF16)
    lower = jnp.concatenate([weights[:half], nothing] * (128 // heads), axis=0)
    upper = jnp.concatenate([nothing, weights[half:]] * (128 // heads), axis=0)
    both = jnp.concatenate([values[: half * head], values[half * head :]], axis=1)
    products = lax.dot_general(
        both, jnp.concatenate([lower, upper], axis=1), (((1,), (1,)), ((), ())), preferred_element_type=F32
    )
    lane = iota((head // 2, 128), 1)
    out = jnp.zeros((head // 2, 128), F32)
    for h in range(half):
        mine = products[h * head : (h + 1) * head]
        out = jnp.where(lane % half == h, jnp.where(lane < heads, mine[: head // 2], mine[head // 2 :]), out)
    return out


def turned(seen):
    rows = seen.T
    half, quarter = rows.shape[0] // 2, rows.shape[0] // 4
    return jnp.concatenate(
        [rows[:quarter], rows[half : half + quarter], rows[quarter:half], rows[half + quarter :]], axis=1
    )


def kernel(
    n,
    q_hbm,
    k_hbm,
    v_hbm,
    out_ref,
    q_ref,
    kbuf,
    vbuf,
    part,
    stat,
    parts,
    stats,
    done,
    q_sem,
    k_sem,
    v_sem,
    part_send,
    stat_send,
    part_recv,
    stat_recv,
    done_send,
    done_recv,
    near_recv,
    last_sem,
):
    me = lax.axis_index("sp")
    cores = 2
    chips = n // cores
    chip, core = lax.div(me, cores), lax.rem(me, cores)
    steps, rows = k_hbm.shape[0], k_hbm.shape[1]
    rounds = steps // chips
    last = steps - 1
    heads = q_ref.shape[0] // (steps * cores)
    head = q_ref.shape[1]

    def chip_of(j):
        away = (chips // 2 - lax.div(j + 1, 2)) * (2 * lax.rem(j, 2) - 1)
        return lax.rem(chip + away + chips, chips)

    def block_of(i):
        return lax.div(i, chips) * chips + chip_of(lax.rem(i, chips))

    def k_copy(i, block=0):
        slot = lax.rem(i, SLOTS)
        return pltpu.make_async_copy(k_hbm.at[block], kbuf.at[slot], k_sem.at[slot])

    def v_copy(i, block=0):
        slot = lax.rem(i, SLOTS)
        return pltpu.make_async_copy(v_hbm.at[block], vbuf.at[slot], v_sem.at[slot])

    def first_copy(j):
        size = rows // cores
        own = pl.ds(j * size, size)
        return pltpu.make_async_copy(k_hbm.at[block_of(0), own], kbuf.at[0, own], last_sem.at[j])

    def rows_of(other):
        size = rows // cores
        return pl.ds(pl.multiple_of(lax.rem(core + other, cores) * size, size), size)

    def last_copy(other):
        return pltpu.make_async_copy(
            v_hbm.at[block_of(last), rows_of(other)], vbuf.at[last % SLOTS, rows_of(other)], last_sem.at[other]
        )

    def send(i, other, r, owner):
        j = i - r * chips
        to = lax.rem(core + other, cores)
        slot = j * cores + 1 - other
        device = {"sp": owner * cores + to}
        pltpu.make_async_remote_copy(
            part.at[i, to],
            parts.at[r, slot],
            part_send,
            part_recv.at[r],
            device_id=device,
            device_id_type=MESH,
        ).start()
        pltpu.make_async_remote_copy(
            stat.at[i, to],
            stats.at[r, slot],
            stat_send,
            stat_recv.at[r],
            device_id=device,
            device_id_type=MESH,
        ).start()

    def score(i, j, block):
        q = q_ref[pl.ds(pl.multiple_of((block * cores + j) * heads, heads), heads), :]
        size = rows // cores
        keys = kbuf.at[lax.rem(i, SLOTS), j * size : (j + 1) * size]
        weights, total, high = weights_of(scores_of(q, keys, head))
        stat[i, j] = jnp.concatenate([total, high], axis=0)
        return weights

    def see(i, j, weights):
        size = rows // cores
        values = vbuf.at[lax.rem(i, SLOTS), j * size : (j + 1) * size]
        part[i, j] = seen_of(weights, values, head).astype(BF16)

    def wait_for(ref, sem):
        pltpu.make_async_copy(ref, ref, sem).wait()

    def finish(r):
        own = n - 1
        parts[r, own] = part[r * chips + chips - 1, core]
        stats[r, own] = stat[r * chips + chips - 1, core]
        wait_for(stats.at[r, : n - 1], stat_recv.at[r])
        highs = [stats[r, t][1:2] for t in range(n)]
        high = functools.reduce(jnp.maximum, highs)
        scales = [jnp.exp(x - high) for x in highs]
        total = functools.reduce(jnp.add, [stats[r, t][0:1] * scales[t] for t in range(n)])
        wait_for(parts.at[r, : n - 1], part_recv.at[r])
        seen = functools.reduce(jnp.add, [parts[r, t].astype(F32) * scales[t] for t in range(n)])
        done[r * n + me] = turned(seen / total).astype(BF16)
        return r * n + me

    def share(which, device, sem):
        pltpu.make_async_remote_copy(
            done.at[which], done.at[which], done_send, sem, device_id={"sp": device}, device_id_type=MESH
        ).start()

    def gather(r):
        for j in range(chips):
            for other in (1, 0):
                if j < chips - 1 or other:
                    share(r * n + me, chip_of(j) * cores + lax.rem(core + other, cores), done_recv.at[r])

    def relay(r):
        partner = chip * cores + lax.rem(core + 1, cores)
        for j in range(chips - 1):
            share(r * n + me, chip_of(j) * cores + core, near_recv.at[j])
            if j == 0:
                share(r * n + me, chip_of(j) * cores + lax.rem(core + 1, cores), done_recv.at[r])
        share(r * n + me, partner, done_recv.at[r])
        for j in reversed(range(chips - 1)):
            wait_for(done.at[0], near_recv.at[j])
            if j > 0:
                away = (chips // 2 - (j + 1) // 2) * (2 * (j % 2) - 1)
                share(r * n + lax.rem(chip - away + chips, chips) * cores + core, partner, done_recv.at[r])

    q_copy = pltpu.make_async_copy(q_hbm, q_ref, q_sem)
    q_copy.start()
    for i in range(SLOTS):
        if i:
            k_copy(i, block_of(i)).start()
        else:
            for j in range(cores):
                first_copy(j).start()
        if i < SLOTS - 1:
            v_copy(i, block_of(i)).start()
    barrier = pltpu.get_barrier_semaphore()
    for away in range(1, n):
        pl.semaphore_signal(barrier, inc=1, device_id={"sp": lax.rem(me + away, n)}, device_id_type=MESH)

    q_copy.wait()
    start = block_of(0)
    weights = []
    for j in range(cores):
        first_copy(j).wait()
        weights.append(score(0, j, start))

    def step(first, i, state):
        blocks, weights = state
        k_copy(i + 1).wait()
        v_copy(i).wait()

        if first:

            @pl.when(i > first)
            def _():
                r = first // chips
                for other in (1, 0):
                    send(i - 1, other, r, blocks[0] - r * chips)

        @pl.when(i + SLOTS < steps)
        def _():
            k_copy(i + SLOTS, blocks[-1]).start()

        @pl.when(i + SLOTS - 1 < last)
        def _():
            v_copy(i + SLOTS - 1, blocks[-2]).start()

        @pl.when(i + SLOTS - 1 == last)
        def _():
            for other in (1, 0):
                last_copy(other).start()

        later = []
        for j in range(cores):
            later.append(score(i + 1, j, blocks[2]))
            see(i, j, weights[j])
        return (*blocks[1:], block_of(lax.rem(i + SLOTS + 1, steps))), tuple(later)

    state = (start, *(block_of(i) for i in range(SLOTS + 1))), tuple(weights)
    state = lax.fori_loop(0, QUIET, functools.partial(step, None), state)
    pl.semaphore_wait(barrier, n - 1)

    def send_both(i, _):
        for other in (1, 0):
            send(i, other, 0, chip_of(i))

    lax.fori_loop(0, QUIET, send_both, None)
    first = QUIET
    for r in range(rounds - 1):
        middle, until = (r + 1) * chips, (r + 1) * chips + EARLY
        state = lax.fori_loop(first, middle, functools.partial(step, first), state)
        send(middle - 1, 1, r, chip)
        state = lax.fori_loop(middle, until, functools.partial(step, middle), state)
        for other in (1, 0):
            send(until - 1, other, r + 1, chip_of(EARLY - 1))
        finish(r)
        gather(r)
        first = until
    _, weights = lax.fori_loop(first, last, functools.partial(step, first), state)
    for other in (1, 0):
        send(last - 1, other, rounds - 1, chip_of(chips - 2))
    mine = [x.astype(F32) for x in weights]
    for other in (1, 0):
        ours = jnp.where(lax.rem(core + other, cores) == 0, *mine).astype(BF16)
        last_copy(other).wait()
        part[last, lax.rem(core + other, cores)] = seen_of(ours, vbuf.at[last % SLOTS, rows_of(other)], head).astype(BF16)
        if other:
            send(last, other, rounds - 1, chip)
    finish(rounds - 1)
    relay(rounds - 1)
    wait_for(parts.at[:, : n - 1], part_send)
    wait_for(stats.at[:, : n - 1], stat_send)
    for r in range(rounds):
        wait_for(done.at[: n - 1], done_send)
    for r in range(rounds - 1):
        wait_for(done.at[: n - 1], done_recv.at[r])
    wait_for(done.at[:chips], done_recv.at[rounds - 1])
    out_ref[...] = done[...]


def unpack(packed_ref, out_ref):
    half, head = packed_ref.shape[1], out_ref.shape[2]
    out_ref[:, :half] = packed_ref[:, :, :head]
    out_ref[:, half:] = packed_ref[:, :, head:]


def solution(mesh):
    n = mesh.shape["sp"]

    def step(q, k, v):
        sequences, tokens, heads, head = k.shape
        steps = sequences // 2
        keys, values = (jnp.transpose(x, (0, 2, 3, 1)).reshape(steps, 2 * heads * head, tokens) for x in (k, v))
        half = head // 2
        rounds = sequences // n
        out = pl.pallas_call(
            functools.partial(kernel, n),
            out_shape=pltpu.VMEM((sequences, heads // 2, 2 * head), BF16),
            in_specs=[pl.BlockSpec(memory_space=pl.ANY)] * 3,
            out_specs=pl.BlockSpec(memory_space=pltpu.VMEM),
            scratch_shapes=[
                pltpu.VMEM((sequences * heads, head), BF16),
                pltpu.VMEM((SLOTS, 2 * heads * head, tokens), BF16),
                pltpu.VMEM((SLOTS, 2 * heads * head, tokens), BF16),
                pltpu.VMEM((steps, 2, half, 2 * heads), BF16),
                pltpu.VMEM((steps, 2, 2, 2 * heads), F32),
                pltpu.VMEM((rounds, n, half, 2 * heads), BF16),
                pltpu.VMEM((rounds, n, 2, 2 * heads), F32),
                pltpu.VMEM((sequences, heads // 2, 2 * head), BF16),
                pltpu.SemaphoreType.DMA(()),
                pltpu.SemaphoreType.DMA((SLOTS,)),
                pltpu.SemaphoreType.DMA((SLOTS,)),
                pltpu.SemaphoreType.DMA(()),
                pltpu.SemaphoreType.DMA(()),
                pltpu.SemaphoreType.DMA((rounds,)),
                pltpu.SemaphoreType.DMA((rounds,)),
                pltpu.SemaphoreType.DMA(()),
                pltpu.SemaphoreType.DMA((rounds,)),
                pltpu.SemaphoreType.DMA((n // 2 - 1,)),
                pltpu.SemaphoreType.DMA((2,)),
            ],
            compiler_params=pltpu.CompilerParams(collective_id=0, has_side_effects=True),
        )(q.reshape(sequences * heads, head), keys, values)
        return pl.pallas_call(
            unpack,
            out_shape=jax.ShapeDtypeStruct(q.shape, BF16),
            in_specs=[pl.BlockSpec(memory_space=pltpu.VMEM)],
            out_specs=pl.BlockSpec(memory_space=pltpu.VMEM),
        )(pltpu.with_memory_space_constraint(out, pltpu.VMEM))

    return jax.shard_map(
        step,
        mesh=mesh,
        in_specs=(P("dp", None, None), P("dp", "sp", None, None), P("dp", "sp", None, None)),
        out_specs=P("dp", None, None),
        check_vma=False,
    )
```

```python
import functools

import jax
import jax.numpy as jnp
from jax import lax
from jax.experimental import pallas as pl
from jax.experimental.pallas import tpu as pltpu
from jax.sharding import PartitionSpec as P

MESH = pl.DeviceIdType.MESH
F32, BF16 = jnp.float32, jnp.bfloat16
SLOTS = 3
QUIET = 4
EARLY = 3
ROWS = 16


def iota(shape, dim):
    return lax.broadcasted_iota(jnp.int32, shape, dim)


def scores_of(q, keys, head):
    heads = q.shape[0]
    per = 128 // head
    out = []
    for first in range(0, heads, ROWS):
        rows = q[first : first + ROWS]
        wide = jnp.concatenate([rows] * per, axis=1)
        blocks = [
            jnp.where(iota((ROWS, 128), 0) == iota((ROWS, 128), 1) // head + per * j, wide, jnp.zeros_like(wide))
            for j in range(ROWS // per)
        ]
        out.append(
            jnp.dot(
                jnp.concatenate(blocks, axis=1),
                keys[first * head : (first + ROWS) * head],
                preferred_element_type=F32,
            )
        )
    return jnp.concatenate(out, axis=0) * head**-0.5


def row_of(column, heads):
    own = iota((heads, 128), 1) % heads == iota((heads, 128), 0)
    return jnp.sum(jnp.where(own, column, 0.0), axis=0, keepdims=True)


def weights_of(scores):
    heads, tokens = scores.shape
    high = jnp.max(scores, axis=1, keepdims=True)
    weights = jnp.exp(scores - high)
    total = jnp.sum(weights, axis=1, keepdims=True)
    wide = lambda x: jnp.broadcast_to(x, (heads, 128))
    return weights.astype(BF16), row_of(wide(total), heads), row_of(wide(high), heads)


def seen_of(weights, values, head):
    heads, tokens = weights.shape
    half = heads // 2
    nothing = jnp.zeros((half, tokens), BF16)
    lower = jnp.concatenate([weights[:half], nothing] * (128 // heads), axis=0)
    upper = jnp.concatenate([nothing, weights[half:]] * (128 // heads), axis=0)
    both = jnp.concatenate([values[: half * head], values[half * head :]], axis=1)
    products = lax.dot_general(
        both, jnp.concatenate([lower, upper], axis=1), (((1,), (1,)), ((), ())), preferred_element_type=F32
    )
    lane = iota((head // 2, 128), 1)
    out = jnp.zeros((head // 2, 128), F32)
    for h in range(half):
        mine = products[h * head : (h + 1) * head]
        out = jnp.where(lane % half == h, jnp.where(lane < heads, mine[: head // 2], mine[head // 2 :]), out)
    return out


def turned(seen):
    rows = seen.T
    half, quarter = rows.shape[0] // 2, rows.shape[0] // 4
    return jnp.concatenate(
        [rows[:quarter], rows[half : half + quarter], rows[quarter:half], rows[half + quarter :]], axis=1
    )


def kernel(
    n,
    q_hbm,
    k_hbm,
    v_hbm,
    out_ref,
    q_ref,
    kbuf,
    vbuf,
    part,
    stat,
    parts,
    stats,
    done,
    q_sem,
    k_sem,
    v_sem,
    part_send,
    stat_send,
    part_recv,
    stat_recv,
    done_send,
    done_recv,
    near_recv,
    last_sem,
):
    me = lax.axis_index("sp")
    cores = 2
    chips = n // cores
    chip, core = lax.div(me, cores), lax.rem(me, cores)
    steps, rows = k_hbm.shape[0], k_hbm.shape[1]
    rounds = steps // chips
    last = steps - 1
    heads = q_ref.shape[0] // (steps * cores)
    head = q_ref.shape[1]

    def chip_of(j):
        away = (chips // 2 - lax.div(j + 1, 2)) * (2 * lax.rem(j, 2) - 1)
        return lax.rem(chip + away + chips, chips)

    def block_of(i):
        return lax.div(i, chips) * chips + chip_of(lax.rem(i, chips))

    def k_copy(i, block=0):
        slot = lax.rem(i, SLOTS)
        return pltpu.make_async_copy(k_hbm.at[block], kbuf.at[slot], k_sem.at[slot])

    def v_copy(i, block=0):
        slot = lax.rem(i, SLOTS)
        return pltpu.make_async_copy(v_hbm.at[block], vbuf.at[slot], v_sem.at[slot])

    def first_copy(j):
        size = rows // cores
        own = pl.ds(j * size, size)
        return pltpu.make_async_copy(k_hbm.at[block_of(0), own], kbuf.at[0, own], last_sem.at[j])

    def rows_of(other):
        size = rows // cores
        return pl.ds(pl.multiple_of(lax.rem(core + other, cores) * size, size), size)

    def last_copy(other):
        return pltpu.make_async_copy(
            v_hbm.at[block_of(last), rows_of(other)], vbuf.at[last % SLOTS, rows_of(other)], last_sem.at[other]
        )

    def send(i, other, r, owner):
        j = i - r * chips
        to = lax.rem(core + other, cores)
        slot = j * cores + 1 - other
        device = {"sp": owner * cores + to}
        pltpu.make_async_remote_copy(
            part.at[i, to],
            parts.at[r, slot],
            part_send,
            part_recv.at[r],
            device_id=device,
            device_id_type=MESH,
        ).start()
        pltpu.make_async_remote_copy(
            stat.at[i, to],
            stats.at[r, slot],
            stat_send,
            stat_recv.at[r],
            device_id=device,
            device_id_type=MESH,
        ).start()

    def score(i, j, block):
        q = q_ref[pl.ds(pl.multiple_of((block * cores + j) * heads, heads), heads), :]
        size = rows // cores
        keys = kbuf.at[lax.rem(i, SLOTS), j * size : (j + 1) * size]
        weights, total, high = weights_of(scores_of(q, keys, head))
        stat[i, j] = jnp.concatenate([total, high], axis=0)
        return weights

    def see(i, j, weights):
        size = rows // cores
        values = vbuf.at[lax.rem(i, SLOTS), j * size : (j + 1) * size]
        part[i, j] = seen_of(weights, values, head).astype(BF16)

    def wait_for(ref, sem):
        pltpu.make_async_copy(ref, ref, sem).wait()

    def finish(r):
        own = n - 1
        parts[r, own] = part[r * chips + chips - 1, core]
        stats[r, own] = stat[r * chips + chips - 1, core]
        wait_for(stats.at[r, : n - 1], stat_recv.at[r])
        highs = [stats[r, t][1:2] for t in range(n)]
        high = functools.reduce(jnp.maximum, highs)
        scales = [jnp.exp(x - high) for x in highs]
        total = functools.reduce(jnp.add, [stats[r, t][0:1] * scales[t] for t in range(n)])
        wait_for(parts.at[r, : n - 1], part_recv.at[r])
        seen = functools.reduce(jnp.add, [parts[r, t].astype(F32) * scales[t] for t in range(n)])
        done[r * n + me] = turned(seen / total).astype(BF16)
        return r * n + me

    def share(which, device, sem):
        pltpu.make_async_remote_copy(
            done.at[which], done.at[which], done_send, sem, device_id={"sp": device}, device_id_type=MESH
        ).start()

    def gather(r):
        for j in range(chips):
            for other in (1, 0):
                if j < chips - 1 or other:
                    share(r * n + me, chip_of(j) * cores + lax.rem(core + other, cores), done_recv.at[r])

    def relay(r):
        partner = chip * cores + lax.rem(core + 1, cores)
        for j in range(chips - 1):
            share(r * n + me, chip_of(j) * cores + core, near_recv.at[j])
            if j == 0:
                share(r * n + me, chip_of(j) * cores + lax.rem(core + 1, cores), done_recv.at[r])
        share(r * n + me, partner, done_recv.at[r])
        for j in reversed(range(chips - 1)):
            wait_for(done.at[0], near_recv.at[j])
            if j > 0:
                away = (chips // 2 - (j + 1) // 2) * (2 * (j % 2) - 1)
                share(r * n + lax.rem(chip - away + chips, chips) * cores + core, partner, done_recv.at[r])

    q_copy = pltpu.make_async_copy(q_hbm, q_ref, q_sem)
    q_copy.start()
    for i in range(SLOTS):
        if i:
            k_copy(i, block_of(i)).start()
        else:
            for j in range(cores):
                first_copy(j).start()
        if i < SLOTS - 1:
            v_copy(i, block_of(i)).start()
    barrier = pltpu.get_barrier_semaphore()
    for away in range(1, n):
        pl.semaphore_signal(barrier, inc=1, device_id={"sp": lax.rem(me + away, n)}, device_id_type=MESH)

    q_copy.wait()
    start = block_of(0)
    weights = []
    for j in range(cores):
        first_copy(j).wait()
        weights.append(score(0, j, start))

    def step(first, i, state):
        blocks, weights = state

        if first:

            @pl.when(i > first)
            def _():
                r = first // chips
                for other in (1, 0):
                    send(i - 1, other, r, blocks[0] - r * chips)

        k_copy(i + 1).wait()
        v_copy(i).wait()

        @pl.when(i + SLOTS < steps)
        def _():
            k_copy(i + SLOTS, blocks[-1]).start()

        @pl.when(i + SLOTS - 1 < last)
        def _():
            v_copy(i + SLOTS - 1, blocks[-2]).start()

        @pl.when(i + SLOTS - 1 == last)
        def _():
            for other in (1, 0):
                last_copy(other).start()

        later = []
        for j in range(cores):
            later.append(score(i + 1, j, blocks[2]))
            see(i, j, weights[j])
        return (*blocks[1:], block_of(lax.rem(i + SLOTS + 1, steps))), tuple(later)

    state = (start, *(block_of(i) for i in range(SLOTS + 1))), tuple(weights)
    state = lax.fori_loop(0, QUIET, functools.partial(step, None), state)
    pl.semaphore_wait(barrier, n - 1)

    def send_both(i, _):
        for other in (1, 0):
            send(i, other, 0, chip_of(i))

    lax.fori_loop(0, QUIET, send_both, None)
    first = QUIET
    for r in range(rounds - 1):
        middle, until = (r + 1) * chips, (r + 1) * chips + EARLY
        state = lax.fori_loop(first, middle, functools.partial(step, first), state)
        send(middle - 1, 1, r, chip)
        state = lax.fori_loop(middle, until, functools.partial(step, middle), state)
        for other in (1, 0):
            send(until - 1, other, r + 1, chip_of(EARLY - 1))
        finish(r)
        gather(r)
        first = until
    _, weights = lax.fori_loop(first, last, functools.partial(step, first), state)
    for other in (1, 0):
        send(last - 1, other, rounds - 1, chip_of(chips - 2))
    mine = [x.astype(F32) for x in weights]
    for other in (1, 0):
        ours = jnp.where(lax.rem(core + other, cores) == 0, *mine).astype(BF16)
        last_copy(other).wait()
        part[last, lax.rem(core + other, cores)] = seen_of(ours, vbuf.at[last % SLOTS, rows_of(other)], head).astype(BF16)
        if other:
            send(last, other, rounds - 1, chip)
    finish(rounds - 1)
    relay(rounds - 1)
    wait_for(parts.at[:, : n - 1], part_send)
    wait_for(stats.at[:, : n - 1], stat_send)
    for r in range(rounds):
        wait_for(done.at[: n - 1], done_send)
    for r in range(rounds - 1):
        wait_for(done.at[: n - 1], done_recv.at[r])
    wait_for(done.at[:chips], done_recv.at[rounds - 1])
    out_ref[...] = done[...]


def unpack(packed_ref, out_ref):
    half, head = packed_ref.shape[1], out_ref.shape[2]
    out_ref[:, :half] = packed_ref[:, :, :head]
    out_ref[:, half:] = packed_ref[:, :, head:]


def solution(mesh):
    n = mesh.shape["sp"]

    def step(q, k, v):
        sequences, tokens, heads, head = k.shape
        steps = sequences // 2
        keys, values = (jnp.transpose(x, (0, 2, 3, 1)).reshape(steps, 2 * heads * head, tokens) for x in (k, v))
        half = head // 2
        rounds = sequences // n
        out = pl.pallas_call(
            functools.partial(kernel, n),
            out_shape=pltpu.VMEM((sequences, heads // 2, 2 * head), BF16),
            in_specs=[pl.BlockSpec(memory_space=pl.ANY)] * 3,
            out_specs=pl.BlockSpec(memory_space=pltpu.VMEM),
            scratch_shapes=[
                pltpu.VMEM((sequences * heads, head), BF16),
                pltpu.VMEM((SLOTS, 2 * heads * head, tokens), BF16),
                pltpu.VMEM((SLOTS, 2 * heads * head, tokens), BF16),
                pltpu.VMEM((steps, 2, half, 2 * heads), BF16),
                pltpu.VMEM((steps, 2, 2, 2 * heads), F32),
                pltpu.VMEM((rounds, n, half, 2 * heads), BF16),
                pltpu.VMEM((rounds, n, 2, 2 * heads), F32),
                pltpu.VMEM((sequences, heads // 2, 2 * head), BF16),
                pltpu.SemaphoreType.DMA(()),
                pltpu.SemaphoreType.DMA((SLOTS,)),
                pltpu.SemaphoreType.DMA((SLOTS,)),
                pltpu.SemaphoreType.DMA(()),
                pltpu.SemaphoreType.DMA(()),
                pltpu.SemaphoreType.DMA((rounds,)),
                pltpu.SemaphoreType.DMA((rounds,)),
                pltpu.SemaphoreType.DMA(()),
                pltpu.SemaphoreType.DMA((rounds,)),
                pltpu.SemaphoreType.DMA((n // 2 - 1,)),
                pltpu.SemaphoreType.DMA((2,)),
            ],
            compiler_params=pltpu.CompilerParams(collective_id=0, has_side_effects=True),
        )(q.reshape(sequences * heads, head), keys, values)
        return pl.pallas_call(
            unpack,
            out_shape=jax.ShapeDtypeStruct(q.shape, BF16),
            in_specs=[pl.BlockSpec(memory_space=pltpu.VMEM)],
            out_specs=pl.BlockSpec(memory_space=pltpu.VMEM),
        )(pltpu.with_memory_space_constraint(out, pltpu.VMEM))

    return jax.shard_map(
        step,
        mesh=mesh,
        in_specs=(P("dp", None, None), P("dp", "sp", None, None), P("dp", "sp", None, None)),
        out_specs=P("dp", None, None),
        check_vma=False,
    )
```
